256 devices in a mesh: gx: 16 (over z, core), gy: 16 (over x, y).
Axes of the slice: x: 4, y: 4, z: 8, core: 2. Of those that a mesh axis runs over, the one named last changes fastest.
Arguments:
- diag_blocks: bfloat16 [128, 128, 128, 128], P('gy', 'gx'), may hold values from -0.13 to 4.25
- edge_blocks: bfloat16 [128, 128, 2, 128, 128], P('gy', 'gx'), may hold values from -1.8 to 0.13
- left_pick: int32 [128, 16], P('gy', 'gx'), may hold values from -4 to 4
- right_pick: int32 [128, 16], P('gy', 'gx'), may hold values from -4 to 4
Outputs:
- pivots: bfloat16 [128, 192, 128, 128], P('gy', 'gx')
- multipliers: bfloat16 [128, 176, 128, 128], P('gy', 'gx')
The draws below stay inside these ranges and needn't reach their ends.
All inputs are finite; a program needn't handle non-finite values.
Results may differ from the reference program's by a relative error of at most 0.0011.
Values may be sent and summed in bfloat16 or wider, within the bound.
No kernel may reach another device: no remote copies, remote signals or barrier semaphores. Data moves between devices by JAX's collectives and lax.ppermute only.
A program may use at most 128 MiB of HBM per device.

```python
import math
import jax
import jax.numpy as jnp
from jax import lax

BLOCK = 128
TILES = 8
REACH = 4
ROWS = 128
TILESG = 128
N_GX = 16


def coupling_fields(key):
    key_tau = jax.random.fold_in(key, 31)
    key_base = jax.random.fold_in(key, 32)
    shape = (ROWS, TILESG, BLOCK)
    tau = jax.random.uniform(key_tau, shape, jnp.float32, 1.2, 1.8)
    base = jnp.exp(jax.random.uniform(key_base, shape, jnp.float32, math.log(0.05), math.log(0.5)))
    return (tau, base)


def draw_diag_blocks(key, part):
    tau, base = coupling_fields(key)
    key_off = jax.random.fold_in(key, 12)
    shape = (ROWS, TILESG, BLOCK, BLOCK)
    spread = 0.02 * jnp.clip(jax.random.normal(key_off, shape, jnp.float32), -6.0, 6.0)
    middle = base + jnp.roll(tau, 1, axis=1) + tau
    eye = jnp.eye(BLOCK, dtype=jnp.float32)
    blocks = spread * (1.0 - eye) + middle[..., None] * eye
    return blocks.astype(jnp.bfloat16)


def draw_edge_blocks(key, part):
    tau, base = coupling_fields(key)
    key_off = jax.random.fold_in(key, 13)
    shape = (ROWS, TILESG, 2, BLOCK, BLOCK)
    spread = 0.02 * jnp.clip(jax.random.normal(key_off, shape, jnp.float32), -6.0, 6.0)
    eye = jnp.eye(BLOCK, dtype=jnp.float32)
    blocks = spread * (1.0 - eye) - tau[:, :, None, :, None] * eye
    return blocks.astype(jnp.bfloat16)


def plant(values, own_key, smallest, top_value):
    spot = [jax.random.randint(jax.random.fold_in(own_key, axis), (), 0, length) for axis, length in enumerate(values.shape)]
    widest = values.shape.index(max(values.shape))
    next_to = spot[:widest] + [(spot[widest] + 1) % values.shape[widest]] + spot[widest + 1:]
    return values.at[tuple(spot)].set(smallest).at[tuple(next_to)].set(top_value)


def setup_inputs(seed: int = 0) -> dict:
    key_list = jax.random.split(jax.random.key(seed), 5)
    return {
        "diag_blocks": draw_diag_blocks(jax.random.fold_in(key_list[4], 71), 0),
        "edge_blocks": draw_edge_blocks(jax.random.fold_in(key_list[4], 71), 0),
        "left_pick": plant(jax.random.randint(key_list[2], (ROWS, N_GX), 0 - REACH, REACH + 1), jax.random.fold_in(key_list[2], 1), 0 - REACH, REACH).astype(jnp.int32),
        "right_pick": plant(jax.random.randint(key_list[3], (ROWS, N_GX), 0 - REACH, REACH + 1), jax.random.fold_in(key_list[3], 1), 0 - REACH, REACH).astype(jnp.int32),
    }


def newton(schur):
    size = schur.shape[-1]
    eye = jnp.eye(size, dtype=schur.dtype)
    inverse_diag = 1.0 / jnp.diagonal(schur, axis1=-2, axis2=-1)
    first = 2.0 * eye * inverse_diag[..., None, :] - inverse_diag[..., :, None] * schur * inverse_diag[..., None, :]
    inner = jnp.einsum("bij,bjk->bik", schur, first, precision=lax.Precision.HIGHEST)
    return 2.0 * first - jnp.einsum("bij,bjk->bik", first, inner, precision=lax.Precision.HIGHEST)


def factor(band_diag, upper, lower):
    start = newton(band_diag[:, 0])

    def advance(previous, items):
        block, up_link, low_link = items
        mult = jnp.einsum("bij,bjk->bik", low_link, previous, precision=lax.Precision.HIGHEST)
        schur = block - jnp.einsum("bij,bjk->bik", mult, up_link, precision=lax.Precision.HIGHEST)
        pivot = newton(schur)
        return pivot, (pivot, mult)

    items = (jnp.moveaxis(band_diag[:, 1:], 1, 0), jnp.moveaxis(upper, 1, 0), jnp.moveaxis(lower, 1, 0))
    _, (later, mults) = lax.scan(advance, start, items)
    pivots = jnp.concatenate([start[:, None], jnp.moveaxis(later, 0, 1)], axis=1)
    return pivots.astype(jnp.bfloat16), jnp.moveaxis(mults, 0, 1).astype(jnp.bfloat16)


def reference(diag_blocks, edge_blocks, left_pick, right_pick):
    lines = jnp.arange(ROWS, dtype=jnp.int32)
    pivot_cols = []
    mult_cols = []
    for column in range(N_GX):
        before = (column - 1) % N_GX
        after = (column + 1) % N_GX
        left_rows = jnp.clip(lines + left_pick[:, column], 0, ROWS - 1).astype(jnp.int32)
        right_rows = jnp.clip(lines + right_pick[:, column], 0, ROWS - 1).astype(jnp.int32)
        low_end = before * TILES + TILES - 2
        left_diag = diag_blocks[:, low_end:low_end + 2][left_rows]
        left_edge = edge_blocks[:, low_end:low_end + 2][left_rows]
        right_diag = diag_blocks[:, after * TILES:after * TILES + 2][right_rows]
        right_edge = edge_blocks[:, after * TILES:after * TILES + 1][right_rows]
        own_diag = diag_blocks[:, column * TILES:(column + 1) * TILES]
        own_edge = edge_blocks[:, column * TILES:(column + 1) * TILES]
        band_diag = jnp.concatenate([left_diag, own_diag, right_diag], axis=1).astype(jnp.float32)
        links = jnp.concatenate([left_edge, own_edge, right_edge], axis=1).astype(jnp.float32)
        pivots, mults = factor(band_diag, links[:, :, 0], links[:, :, 1])
        pivot_cols.append(pivots)
        mult_cols.append(mults)
    return jnp.concatenate(pivot_cols, axis=1), jnp.concatenate(mult_cols, axis=1)
```

```python
import functools
import jax
import jax.numpy as jnp
from jax import lax
from jax.experimental import pallas as pl
from jax.experimental.pallas import tpu as pltpu
from jax.sharding import PartitionSpec as P


F32 = jnp.float32
BF16 = jnp.bfloat16


def split(x):
    hi = x.astype(BF16)
    return hi, (x - hi.astype(F32)).astype(BF16)


def dot(a, b):
    return jnp.dot(a, b, preferred_element_type=F32)


def eye_mask(n):
    return lax.broadcasted_iota(jnp.int32, (n, n), 0) == lax.broadcasted_iota(jnp.int32, (n, n), 1)


def cost(us):
    return pl.CostEstimate(flops=us * 10**8, bytes_accessed=10**6, transcendentals=0)


class Stages:
    def __init__(self, lines, size, refs):
        self.lines = lines
        self.size = size
        self.ph, self.pl, self.mh, self.ml, self.fh, self.fl, self.q, self.dc = refs

    def scale(self, i, s):
        eye = eye_mask(self.size)
        on = jnp.where(eye, s, 0.0)
        drow = 1.0 / jnp.sum(on, axis=0, keepdims=True)
        dcol = 1.0 / jnp.sum(on, axis=1, keepdims=True)
        fh, fl = split(jnp.where(eye, 0.0, s) * drow)
        self.fh[i] = fh
        self.fl[i] = fl
        self.dc[i] = jnp.broadcast_to(dcol, s.shape)

    def square(self, i):
        fh = self.fh[i]
        fl = self.fl[i]
        g = dot(fh, fh) + dot(fh, fl) + dot(fl, fh)
        gh, gl = split(g)
        eye = jnp.where(eye_mask(self.size), 1.0, 0.0)
        self.q[i] = eye - fh.astype(F32) - fl.astype(F32) + g
        self.mh[i] = gh
        self.ml[i] = gl

    def finish(self, i, out):
        fh = self.fh[i]
        fl = self.fl[i]
        gh = self.mh[i]
        gl = self.ml[i]
        h = dot(fh, gh) + dot(fl, gh) + dot(fh, gl)
        p = self.dc[i] * (self.q[i] - h)
        hi, lo = split(p)
        self.ph[i] = hi
        self.pl[i] = lo
        out(i, hi)

    def newton(self, schur, out):
        for i in range(self.lines):
            self.scale(i, schur(i))
        for i in range(self.lines):
            self.square(i)
        for i in range(self.lines):
            self.finish(i, out)

    def mult(self, lower, out):
        for i in range(self.lines):
            low = lower(i)
            m = dot(low, self.ph[i]) + dot(low, self.pl[i])
            hi, lo = split(m)
            self.mh[i] = hi
            self.ml[i] = lo
            out(i, hi)

    def update(self, i, up):
        return dot(self.mh[i], up) + dot(self.ml[i], up)


def stage_scratch(lines, n):
    return [pltpu.VMEM((lines, n, n), BF16)] * 6 + [pltpu.VMEM((lines, n, n), F32)] * 2


def start_kernel(lines, n, tiles, diag, edge, tm, tt, tb, pm, pt, pb, rm, rt, rb,
                 dv, ev, pmv, tv, rv, isem, rsem, osem, *refs):
    st = Stages(lines, n, refs)
    h = lines // 2
    dc = [pltpu.make_async_copy(diag.at[:, tiles - 2 + k], dv.at[k], isem.at[k]) for k in range(2)]
    ec = [pltpu.make_async_copy(edge.at[:, tiles - 2 + k], ev.at[k], isem.at[k + 2]) for k in range(2)]
    rc = [pltpu.make_async_copy(diag.at[:, 0:2], rv.at[:, 0:2], rsem.at[0]),
          pltpu.make_async_copy(edge.at[:, 0], rv.at[:, 2:4], rsem.at[1])]
    for c in (dc[0], ec[0], dc[1], ec[1], rc[0], rc[1]):
        c.start()

    def put(slot):
        def out(i, x):
            pmv[i, slot] = x

        return out

    outs = [pltpu.make_async_copy(s, d, osem.at[j]) for j, (s, d) in enumerate((
        (rv, rm), (rv.at[:h], rt), (rv.at[h:], rb),
        (tv, tm), (tv.at[:h], tt), (tv.at[h:], tb),
        (pmv, pm), (pmv.at[:h], pt), (pmv.at[h:], pb)))]
    dc[0].wait()
    st.newton(lambda i: dv[0, i].astype(F32), put(0))
    ec[0].wait()
    st.mult(lambda i: ev[0, i, 1], put(2))
    rc[0].wait()
    rc[1].wait()
    for c in outs[:3]:
        c.start()
    dc[1].wait()
    st.newton(lambda i: dv[1, i].astype(F32) - st.update(i, ev[0, i, 0]), put(1))
    ec[1].wait()
    st.mult(lambda i: ev[1, i, 1], put(3))
    for i in range(lines):
        tv[i, 0], tv[i, 1] = split(st.update(i, ev[1, i, 0]))
    for c in outs[3:]:
        c.start()
    for c in outs:
        c.wait()


def source(pick, i, lines):
    first = lax.axis_index("gy") * lines
    return jnp.clip(first + i + pick[i], 0, lax.axis_size("gy") * lines - 1) - first


def fetch(at, h, lines, main, prev, nxt, dst, sem):
    @pl.when(at < 0)
    def _():
        pltpu.make_async_copy(prev(jnp.clip(at + h, 0, h - 1)), dst, sem).start()

    @pl.when((at >= 0) & (at < lines))
    def _():
        pltpu.make_async_copy(main(jnp.clip(at, 0, lines - 1)), dst, sem).start()

    @pl.when(at >= lines)
    def _():
        pltpu.make_async_copy(nxt(jnp.clip(at - lines, 0, h - 1)), dst, sem).start()


def middle_kernel(lines, n, tiles, pick, tm, tp, tn, diag, edge, piv, mul, v, dv, ev, win, pv, mv, vv,
                  dsem, esem, tsem, osem, vsem, *refs):
    st = Stages(lines, n, refs)
    h = lines // 2

    def dcopy(k):
        return pltpu.make_async_copy(diag.at[:, k], dv.at[k], dsem.at[k])

    def ecopy(k):
        return pltpu.make_async_copy(edge.at[:, k], ev.at[k], esem.at[k])

    def pcopy(k):
        return pltpu.make_async_copy(pv.at[k], piv.at[:, k + 2], osem.at[0, k])

    def mcopy(k):
        return pltpu.make_async_copy(mv.at[k], mul.at[:, k + 2], osem.at[1, k])

    dcopy(0).start()
    for i in range(lines):
        fetch(source(pick, i, lines), h, lines, lambda r: tm.at[r], lambda r: tp.at[r],
              lambda r: tn.at[r], win.at[i], tsem.at[i])
    for k in range(tiles):
        if k:
            dcopy(k).start()
        ecopy(k).start()
    dcopy(0).wait()
    for i in range(lines):
        pltpu.make_async_copy(tm.at[0], win.at[i], tsem.at[i]).wait()

    def put(buf, k):
        def out(i, x):
            buf[k, i] = x

        return out

    st.newton(lambda i: dv[0, i].astype(F32) - win[i, 0].astype(F32) - win[i, 1].astype(F32), put(pv, 0))

    def step(k, _):
        ecopy(k - 1).wait()
        st.mult(lambda i: ev[k - 1, i, 1], put(mv, k - 1))
        pcopy(k - 1).start()
        dcopy(k).wait()
        st.newton(lambda i: dv[k, i].astype(F32) - st.update(i, ev[k - 1, i, 0]), put(pv, k))
        mcopy(k - 1).start()
        return 0

    lax.fori_loop(1, tiles, step, 0)
    ecopy(tiles - 1).wait()
    st.mult(lambda i: ev[tiles - 1, i, 1], put(mv, tiles - 1))
    pcopy(tiles - 1).start()
    for i in range(lines):
        vv[i] = st.update(i, ev[tiles - 1, i, 0])
    mcopy(tiles - 1).start()
    vc = pltpu.make_async_copy(vv, v, vsem)
    vc.start()
    for k in range(tiles):
        pcopy(k).wait()
        mcopy(k).wait()
    vc.wait()


HBM = pl.BlockSpec(memory_space=pltpu.HBM)
SMEM = pl.BlockSpec(memory_space=pltpu.SMEM)
VMEM = pl.BlockSpec(memory_space=pltpu.VMEM)
LIMIT = 67043328


def middle(pick, tm, tp, tn, diag, edge):
    lines, tiles, n, _ = diag.shape
    return pl.pallas_call(
        functools.partial(middle_kernel, lines, n, tiles),
        out_shape=(jax.ShapeDtypeStruct((lines, tiles + 4, n, n), BF16),
                   jax.ShapeDtypeStruct((lines, tiles + 3, n, n), BF16),
                   jax.ShapeDtypeStruct((lines, n, n), F32)),
        in_specs=[SMEM] + [HBM] * 5,
        out_specs=(HBM,) * 3,
        scratch_shapes=[
            pltpu.VMEM((tiles, lines, n, n), BF16),
            pltpu.VMEM((tiles, lines, 2, n, n), BF16),
            pltpu.VMEM((lines, 2, n, n), BF16),
            pltpu.VMEM((tiles, lines, n, n), BF16),
            pltpu.VMEM((tiles, lines, n, n), BF16),
            pltpu.VMEM((lines, n, n), F32),
            pltpu.SemaphoreType.DMA((tiles,)),
            pltpu.SemaphoreType.DMA((tiles,)),
            pltpu.SemaphoreType.DMA((lines,)),
            pltpu.SemaphoreType.DMA((2, tiles)),
            pltpu.SemaphoreType.DMA,
        ] + stage_scratch(lines, n),
        compiler_params=pltpu.CompilerParams(vmem_limit_bytes=LIMIT),
        cost_estimate=cost(14),
        name="middle",
    )(pick, tm, tp, tn, diag, edge)


def start(diag, edge):
    lines, tiles, n, _ = diag.shape
    h = lines // 2
    shapes = [(lines, 2), (h, 2), (h, 2)] + [(lines, 4), (h, 4), (h, 4)] * 2
    return pl.pallas_call(
        functools.partial(start_kernel, lines, n, tiles),
        out_shape=tuple(jax.ShapeDtypeStruct((*s, n, n), BF16) for s in shapes),
        in_specs=[HBM] * 2,
        out_specs=(HBM,) * 9,
        scratch_shapes=[
            pltpu.VMEM((2, lines, n, n), BF16),
            pltpu.VMEM((2, lines, 2, n, n), BF16),
            pltpu.VMEM((lines, 4, n, n), BF16),
            pltpu.VMEM((lines, 2, n, n), BF16),
            pltpu.VMEM((lines, 4, n, n), BF16),
            pltpu.SemaphoreType.DMA((4,)),
            pltpu.SemaphoreType.DMA((2,)),
            pltpu.SemaphoreType.DMA((9,)),
        ] + stage_scratch(lines, n),
        compiler_params=pltpu.CompilerParams(vmem_limit_bytes=LIMIT),
        cost_estimate=cost(5),
        name="start",
    )(diag, edge)


def end_kernel(lines, n, tiles, pickl, pickr, v, rm, rp, rn, pm, pp, pn, piv0, mul0, piv, mul,
               vv, rv, pmv, pv, mv, vsem, rsem, psem, osem, bsem, *refs):
    st = Stages(lines, n, refs)
    h = lines // 2
    vc = pltpu.make_async_copy(v, vv, vsem)
    vc.start()
    for i in range(lines):
        fetch(source(pickr, i, lines), h, lines, lambda r: rm.at[r], lambda r: rp.at[r],
              lambda r: rn.at[r], rv.at[i], rsem.at[i])
    for i in range(lines):
        fetch(source(pickl, i, lines), h, lines, lambda r: pm.at[r], lambda r: pp.at[r],
              lambda r: pn.at[r], pmv.at[i], psem.at[i])
    vc.wait()
    for i in range(lines):
        pltpu.make_async_copy(rm.at[0], rv.at[i], rsem.at[i]).wait()

    def put(buf, k):
        def out(i, x):
            buf[k, i] = x

        return out

    st.newton(lambda i: rv[i, 0].astype(F32) - vv[i], put(pv, 0))
    outs = []
    for i in range(lines):
        pltpu.make_async_copy(pm.at[0], pmv.at[i], psem.at[i]).wait()
        outs.append(pltpu.make_async_copy(pmv.at[i, 0:2], piv.at[i, 0:2], bsem.at[0, i]))
        outs.append(pltpu.make_async_copy(pmv.at[i, 2:4], mul.at[i, 0:2], bsem.at[1, i]))
        outs[-2].start()
        outs[-1].start()
    st.mult(lambda i: rv[i, 3], put(mv, 0))
    outs.append(pltpu.make_async_copy(pv.at[0], piv.at[:, tiles + 2], osem.at[0]))
    outs[-1].start()
    st.newton(lambda i: rv[i, 1].astype(F32) - st.update(i, rv[i, 2]), put(pv, 1))
    outs.append(pltpu.make_async_copy(mv.at[0], mul.at[:, tiles + 2], osem.at[1]))
    outs[-1].start()
    outs.append(pltpu.make_async_copy(pv.at[1], piv.at[:, tiles + 3], osem.at[2]))
    outs[-1].start()
    for c in outs:
        c.wait()


def end(pickl, pickr, v, rm, rp, rn, pm, pp, pn, piv, mul):
    lines, n, _ = v.shape
    tiles = piv.shape[1] - 4
    return pl.pallas_call(
        functools.partial(end_kernel, lines, n, tiles),
        out_shape=(jax.ShapeDtypeStruct(piv.shape, BF16), jax.ShapeDtypeStruct(mul.shape, BF16)),
        in_specs=[SMEM] * 2 + [HBM] * 9,
        out_specs=(HBM,) * 2,
        input_output_aliases={9: 0, 10: 1},
        scratch_shapes=[
            pltpu.VMEM((lines, n, n), F32),
            pltpu.VMEM((lines, 4, n, n), BF16),
            pltpu.VMEM((lines, 4, n, n), BF16),
            pltpu.VMEM((2, lines, n, n), BF16),
            pltpu.VMEM((1, lines, n, n), BF16),
            pltpu.SemaphoreType.DMA,
            pltpu.SemaphoreType.DMA((lines,)),
            pltpu.SemaphoreType.DMA((lines,)),
            pltpu.SemaphoreType.DMA((3,)),
            pltpu.SemaphoreType.DMA((2, lines)),
        ] + stage_scratch(lines, n),
        compiler_params=pltpu.CompilerParams(vmem_limit_bytes=LIMIT),
        cost_estimate=cost(5),
        name="end",
    )(pickl, pickr, v, rm, rp, rn, pm, pp, pn, piv, mul)


def moved(array, gy, gx):
    ny, nx = lax.axis_size("gy"), lax.axis_size("gx")
    pairs = [(x * ny + y, (x + gx) % nx * ny + (y + gy) % ny) for x in range(nx) for y in range(ny)]
    return lax.ppermute(array, ("gx", "gy"), pairs)


def on_device(diag, edge, left_pick, right_pick):
    left_pick, right_pick = left_pick.reshape(-1), right_pick.reshape(-1)
    t, tt, tb, out4, out4t, out4b, right, rt, rb = start(diag, edge)
    tm, tp, tn = moved(t, 0, 1), moved(tb, 1, 1), moved(tt, -1, 1)
    pm, pp, pn = moved(out4, 0, 1), moved(out4b, 1, 1), moved(out4t, -1, 1)
    rm, rp, rn = moved(right, 0, -1), moved(rb, 1, -1), moved(rt, -1, -1)
    piv, mul, v = middle(left_pick, tm, tp, tn, diag, edge)
    return end(left_pick, right_pick, v, rm, rp, rn, pm, pp, pn, piv, mul)


def solution(mesh):
    return jax.shard_map(
        on_device,
        mesh=mesh,
        in_specs=(
            P("gy", "gx", None, None),
            P("gy", "gx", None, None, None),
            P("gy", "gx"),
            P("gy", "gx"),
        ),
        out_specs=(P("gy", "gx", None, None), P("gy", "gx", None, None)),
        check_vma=False,
    )
```
